32 devices in a mesh: groups: 2 (over y), pool: 8 (over z, x), heads: 2 (over core).
Axes of the slice: x: 2, y: 2, z: 4, core: 2. Of those that a mesh axis runs over, the one named last changes fastest.
Arguments:
- hidden_in: bfloat16 [32, 8192], P('groups'), parts along dimension 0, may hold values from -50 to 50
- key_cache: bfloat16 [32, 8, 4096, 128], P('groups', 'heads', 'pool'), parts along dimension 0, may hold values from -200 to 200
- value_cache: bfloat16 [32, 8, 4096, 128], P('groups', 'heads', 'pool'), parts along dimension 0, may hold values from -6 to 6
- positions: int32 [3, 32, 4096], P(None, 'groups', 'pool'), parts along dimension 1, may hold values from 0 to 4095, as said below
- query_pos: int32 [3, 32], P(None, 'groups'), parts along dimension 1, may hold values from 4096 to 8207
- lengths: int32 [32], P('groups'), parts along dimension 0, may hold values from 1024 to 4096, as said below
- query_weight: bfloat16 [8192, 8192], P('pool', 'heads'), may hold values from -0.0625 to 0.0625
- key_weight: bfloat16 [8192, 1024], P('pool', 'heads'), may hold values from -0.16503906 to 0.16503906
- value_weight: bfloat16 [8192, 1024], P('pool', 'heads'), may hold values from -0.16503906 to 0.16503906
- out_weight: bfloat16 [8192, 8192], P('heads', 'pool'), may hold values from -0.5 to 0.5
- gate_weight: bfloat16 [8192, 14848], P(None, ('pool', 'heads')), may hold values from -0.0625 to 0.0625
- up_weight: bfloat16 [8192, 14848], P(None, ('pool', 'heads')), may hold values from -0.0625 to 0.0625
- down_weight: bfloat16 [14848, 8192], P(('pool', 'heads')), may hold values from -0.0625 to 0.0625
Outputs:
- output: bfloat16 [32, 8192], P('groups', 'pool'), parts along dimension 0
The draws below stay inside these ranges and needn't reach their ends.
There are 2 independent parts, one for each index of `groups`. The reference program is written for one: setup_inputs(seed, part) draws one part's arguments, and reference() takes and returns one part's arrays. A program takes and returns all parts, laid end to end along the dimension named above; an argument that names none is the same for every part. Nothing has to cross between parts.
Inputs may be any that keep to these rules, and one draw needn't show every extreme that they name: `positions`: text tokens carry three equal ids; one prompt is text only. `lengths`: some prompt fills all 4096 slots.
All inputs are finite; a program needn't handle non-finite values.
Results may differ from the reference program's by a relative error of at most 0.007.
The reference program's roundings to bfloat16 on the way count: a program that leaves them out, or rounds other values in their place, can miss the bound.
Values may be sent and summed in bfloat16 or wider, within the bound.
A program may use at most 192 MiB of HBM per device.

```python
import math
import jax
import jax.numpy as jnp
from jax import lax

D = 8192
HEADS = 64
KV_HEADS = 8
HD = 128
FF = 14848
PROMPTS = 16
SEQ = 4096


def draw_hidden_in(key, part):
    subkeys = jax.random.split(jax.random.fold_in(key, 11), 3)
    values_base = jax.random.truncated_normal(subkeys[0], -4.0, 4.0, (PROMPTS, D), jnp.float32)
    row_scale = jnp.exp(jax.random.uniform(subkeys[1], (PROMPTS, 1), jnp.float32, 0.0, math.log(4.0)))
    rise = math.log(10.0)
    column = jnp.arange(D).astype(jnp.float32) / D
    col_scale = jnp.exp(rise * (column - 0.5) + jax.random.uniform(subkeys[2], (D,), jnp.float32, -0.4, 0.4))
    return jnp.clip(values_base * row_scale * col_scale[None, :], -50.0, 50.0).astype(jnp.bfloat16)


def draw_key_cache(key, part):
    subkeys = jax.random.split(jax.random.fold_in(key, 53), 4)
    full_shape = (PROMPTS, KV_HEADS, SEQ, HD)
    base_values = 2.0 * jax.random.truncated_normal(subkeys[0], -6.0, 6.0, full_shape, jnp.float32)
    strength = jnp.exp(jax.random.uniform(subkeys[1], (PROMPTS, KV_HEADS, 1, 1), jnp.float32, math.log(30.0), math.log(200.0)))
    pattern = jax.random.rademacher(subkeys[2], (PROMPTS, KV_HEADS, 1, HD), jnp.float32)
    slot_choice = jax.random.randint(subkeys[3], (3, PROMPTS, KV_HEADS, 1, 1), 0, SEQ // 4)
    slot_index = jnp.arange(SEQ).reshape(1, 1, SEQ, 1)
    drawn = base_values
    for planted_index, factor in enumerate((1.0, 0.99, 0.98)):
        drawn = jnp.where(slot_index == slot_choice[planted_index], factor * strength * pattern, drawn)
    return jnp.clip(drawn, -200.0, 200.0).astype(jnp.bfloat16)


def draw_positions(key, part):
    subkeys = jax.random.split(jax.random.fold_in(key, 23), 3)
    text_len = jax.random.randint(subkeys[0], (PROMPTS,), 4, max(5, SEQ // 4))
    step_size = jax.random.randint(subkeys[1], (PROMPTS,), 1, 5)
    text_prompt = jax.random.randint(subkeys[2], (), 0, PROMPTS)
    token_index = jnp.arange(SEQ)[None, :]
    offset = token_index - text_len[:, None]
    in_video = (offset >= 0) & (jnp.arange(PROMPTS)[:, None] != text_prompt)
    clamped = jnp.maximum(offset, 0)
    frame = clamped // 64
    patch_row = clamped % 64 // 8
    patch_col = clamped % 8
    temporal = jnp.where(in_video, text_len[:, None] + frame * step_size[:, None], token_index)
    height = jnp.where(in_video, text_len[:, None] + patch_row, token_index)
    width = jnp.where(in_video, text_len[:, None] + patch_col, token_index)
    return jnp.clip(jnp.stack([temporal, height, width]), 0, SEQ - 1).astype(jnp.int32)


def draw_query_pos(key, part):
    subkeys = jax.random.split(jax.random.fold_in(key, 37), 2)
    anchor = jax.random.randint(subkeys[0], (1, PROMPTS), SEQ, 2 * SEQ)
    extra = jax.random.randint(subkeys[1], (3, PROMPTS), 0, 16)
    return (anchor + extra).astype(jnp.int32)


def draw_lengths(key, part):
    subkeys = jax.random.split(jax.random.fold_in(key, 41), 2)
    drawn = jax.random.randint(subkeys[0], (PROMPTS,), SEQ // 4, SEQ + 1)
    chosen = jax.random.randint(subkeys[1], (), 0, PROMPTS)
    return drawn.at[chosen].set(SEQ).astype(jnp.int32)


def spiked(values, rng, source, target, shards_of, factor):
    def block_of(axis_at):
        return (jnp.arange(values.shape[axis_at]) // (values.shape[axis_at] // shards_of)).reshape((-1,) + (1,) * (values.ndim - 1 - axis_at))

    one_side = jax.random.permutation(rng, shards_of)[block_of(target)]
    far = (block_of(target) + shards_of // 2) % shards_of
    return jnp.where((block_of(source) == one_side) | (block_of(source) == far), factor * values, values)


def block_levels(rng, shape, shards, low, high):
    gain, own = 1.0, jax.random.fold_in(rng, 6)
    for axis_at, shards_of in shards:
        draws = jnp.exp(jax.random.uniform(jax.random.fold_in(own, axis_at), (shards_of,), jnp.float32, low / len(shards), high / len(shards)))
        gain = gain * jnp.repeat(draws, shape[axis_at] // shards_of).reshape([-1 if axis == axis_at else 1 for axis in range(len(shape))])
    return gain


def centred(rng, dims, spread, most, shards=(), held_as=jnp.bfloat16):
    values = spread * jax.random.normal(rng, dims, jnp.float32)
    if shards:
        values = values * block_levels(rng, dims, shards, -0.22, 0.18)
    return jnp.clip(values, -most, most).astype(held_as)


def bell_draw_with(own_key, shape, spread, reach, shards, heavy, dtype=jnp.bfloat16):
    values = spread * jax.random.normal(own_key, shape, jnp.float32)
    if shards:
        values = values * block_levels(own_key, shape, shards, -0.22, 0.18)
    return jnp.clip(spiked(values, jax.random.fold_in(own_key, 3), *heavy), -reach, reach).astype(dtype)


def setup_inputs(seed: int = 0, part: int = 0) -> dict:
    arg_keys = jax.random.split(jax.random.key(seed), 14)
    part_keys = jax.random.split(jax.random.fold_in(arg_keys[13], part), 14)
    return {
        "hidden_in": draw_hidden_in(jax.random.fold_in(jax.random.fold_in(arg_keys[13], part), 71), part),
        "key_cache": draw_key_cache(jax.random.fold_in(jax.random.fold_in(arg_keys[13], part), 71), part),
        "value_cache": centred(part_keys[2], (PROMPTS, KV_HEADS, SEQ, HD), 1.0, 6.0, ((1, 2), (2, 8))),
        "positions": draw_positions(jax.random.fold_in(jax.random.fold_in(arg_keys[13], part), 71), part),
        "query_pos": draw_query_pos(jax.random.fold_in(jax.random.fold_in(arg_keys[13], part), 71), part),
        "lengths": draw_lengths(jax.random.fold_in(jax.random.fold_in(arg_keys[13], part), 71), part),
        "query_weight": centred(arg_keys[6], (D, HEADS * HD), D ** -0.5, 0.0625, ((0, 8), (1, 2))),
        "key_weight": centred(arg_keys[7], (D, KV_HEADS * HD), (2.5 / D ** 0.5), 0.16503906, ((0, 8), (1, 2))),
        "value_weight": centred(arg_keys[8], (D, KV_HEADS * HD), (2.5 / D ** 0.5), 0.16503906, ((0, 8), (1, 2))),
        "out_weight": centred(arg_keys[9], (HEADS * HD, D), HD ** -0.5, 0.5, ((0, 2), (1, 8))),
        "gate_weight": centred(arg_keys[10], (D, FF), D ** -0.5, 0.0625, ((1, 16),)),
        "up_weight": centred(arg_keys[11], (D, FF), D ** -0.5, 0.0625, ((1, 16),)),
        "down_weight": bell_draw_with(arg_keys[12], (FF, D), FF ** -0.5, 0.0625, ((0, 16),), (0, 1, 16, 2.0)),
    }


EPS = 1e-06
THETA = 1000000.0

def angle_tables(triple):
    half_dim = HD // 2
    column = jnp.arange(half_dim)
    first_end = HD // 8
    second_end = first_end + 3 * HD // 16
    chosen = jnp.where(column < first_end, triple[0][..., None], jnp.where(column < second_end, triple[1][..., None], triple[2][..., None]))
    inverse = jnp.exp(column.astype(jnp.float32) * (-2.0 * math.log(THETA) / HD))
    angles = chosen.astype(jnp.float32) * inverse
    return (jnp.cos(angles), jnp.sin(angles))

def rotate(values, cos_table, sin_table):
    half_dim = values.shape[-1] // 2
    lower_half = values[..., :half_dim]
    upper_half = values[..., half_dim:]
    return jnp.concatenate([lower_half * cos_table - upper_half * sin_table, upper_half * cos_table + lower_half * sin_table], -1)

def normalize(values):
    return values * lax.rsqrt(lax.optimization_barrier(jnp.mean(values * values, -1, keepdims=True)) + EPS)

def reference(hidden_in, key_cache, value_cache, positions, query_pos, lengths, query_weight, key_weight, value_weight, out_weight, gate_weight, up_weight, down_weight):
    group_size = HEADS // KV_HEADS
    score_scale = HD ** (-0.5)
    normed = normalize(hidden_in.astype(jnp.float32)).astype(jnp.bfloat16)
    raw_queries = jnp.dot(normed, query_weight, preferred_element_type=jnp.float32).reshape(PROMPTS, HEADS, HD)
    raw_keys = jnp.dot(normed, key_weight, preferred_element_type=jnp.float32).reshape(PROMPTS, KV_HEADS, HD)
    new_values = jnp.dot(normed, value_weight, preferred_element_type=jnp.float32).reshape(PROMPTS, KV_HEADS, HD).astype(jnp.bfloat16)
    query_cos, query_sin = angle_tables(query_pos)
    queries = rotate(raw_queries, query_cos[:, None], query_sin[:, None]).astype(jnp.bfloat16)
    own_keys = rotate(raw_keys, query_cos[:, None], query_sin[:, None]).astype(jnp.bfloat16)

    def attend_prompt(inputs):
        query_rows, key_new, value_new, cached_keys, cached_values, triple, length = inputs
        cos_table, sin_table = angle_tables(triple)
        rotated = rotate(cached_keys.astype(jnp.float32), cos_table[None], sin_table[None]).astype(jnp.bfloat16)
        grouped = query_rows.reshape(KV_HEADS, group_size, HD).astype(jnp.float32)
        scores = jnp.einsum('kgd,ksd->kgs', grouped, rotated.astype(jnp.float32)) * score_scale
        valid_mask = jnp.arange(SEQ) < length
        scores = jnp.where(valid_mask, scores, -1e+30)
        own_score = jnp.einsum('kgd,kd->kg', grouped, key_new.astype(jnp.float32)) * score_scale
        peak_score = jnp.maximum(lax.optimization_barrier(jnp.max(scores, -1)), own_score)
        weights = jnp.where(valid_mask, jnp.exp(scores - peak_score[..., None]), 0.0)
        own_weight = jnp.exp(own_score - peak_score)
        denominator = lax.optimization_barrier(jnp.sum(weights, -1)) + own_weight
        blended = jnp.einsum('kgs,ksd->kgd', weights, cached_values.astype(jnp.float32))
        blended = blended + own_weight[..., None] * value_new.astype(jnp.float32)[:, None, :]
        return (blended / denominator[..., None]).reshape(HEADS * HD).astype(jnp.bfloat16)
    triples = jnp.transpose(positions, (1, 0, 2))
    attended = lax.map(attend_prompt, (queries, own_keys, new_values, key_cache, value_cache, triples, lengths))
    attn_out = jnp.dot(attended, out_weight, preferred_element_type=jnp.float32)
    mid_state = (hidden_in.astype(jnp.float32) + attn_out).astype(jnp.bfloat16)
    normed_state = normalize(mid_state.astype(jnp.float32)).astype(jnp.bfloat16)
    gate_values = jnp.dot(normed_state, gate_weight, preferred_element_type=jnp.float32)
    up_values = jnp.dot(normed_state, up_weight, preferred_element_type=jnp.float32)
    active = (jax.nn.silu(gate_values) * up_values).astype(jnp.bfloat16)
    down_values = jnp.dot(active, down_weight, preferred_element_type=jnp.float32)
    return (mid_state.astype(jnp.float32) + down_values).astype(jnp.bfloat16)
```

```python
import functools
import math

import jax
import jax.numpy as jnp
from jax import lax
from jax.experimental import pallas as pl
from jax.experimental.pallas import tpu as pltpu
from jax.sharding import PartitionSpec as P

HD = 128
EPS = 1e-06
THETA = 1000000.0
MESH = pl.DeviceIdType.MESH
F32 = jnp.float32
BF16 = jnp.bfloat16

TURN_A = 6.28125
TURN_B = round((2 * math.pi - TURN_A) * 2**20) / 2**20
TURN_C = 2 * math.pi - TURN_A - TURN_B
SINE = [(-1) ** i / math.factorial(2 * i + 1) for i in range(7)]


def rope_tables(ids, inverse, lane):
    angle = ids * inverse
    upper = lane >= HD // 2
    quarter = jnp.where(upper, 0.25, 0.0).astype(F32)
    turns = jnp.floor(angle * (1.0 / (2 * math.pi)) - quarter + 0.5)
    rest = angle - turns * TURN_A
    rest = rest - turns * TURN_B
    rest = rest - turns * TURN_C
    half = (rest - quarter * (2 * math.pi)) * 0.5
    square = half * half
    poly = jnp.full_like(square, SINE[6])
    for i in range(5, -1, -1):
        poly = poly * square + SINE[i]
    sine = poly * half
    table = 1.0 - 2.0 * sine * sine
    swapped = pltpu.roll(table, HD // 2, 1)
    cos_table = jnp.where(upper, swapped, table)
    sin_table = jnp.where(upper, table, -swapped)
    return cos_table, sin_table


def make_kernel(n, prompts, lh, seq, d_model, ffl, group, wb, nslots, vslots, share):
    cb = d_model // n
    items = prompts * lh
    ipd = items // n
    per_head = prompts // ipd
    qw = group * HD
    cols = group + 2
    half_rows = prompts // 2
    nblocks = d_model // wb
    scale = HD ** (-0.5)

    def kernel(
        hidden, posx, sel, qsel, inv, lens, key_hbm, val_hbm, wq, wk, wv, wo, wg, wu, wd,
        out_ref,
        kbuf, vbuf, qkvbuf, wobuf, wgbuf, wubuf, chunk, chunk_in, tr, qg, acc, acc_in, ml, ml_in,
        atf, ats, atg, part, part_in, midf, mid_send, mg, ns, dpart, dother, ssum, rsum, yb, tabs,
        wsem, ksem, vsem, bigsem, dsem,
        s1, r1, s2, r2, s3, r3, s4, r4, s5, r5, s6, r6, s7, r7, s8, r8, hs, hr,
        *maybe_down,
    ):
        me = lax.axis_index("pool")
        hd = lax.axis_index("heads")
        other = 1 - hd

        def block_slot(b):
            buf = qkvbuf if share else maybe_down[0]
            slot = lax.rem(b, nslots)
            return buf.at[slot, pl.ds(0, ffl)] if share else buf.at[slot]

        def down_copy(b):
            return pltpu.make_async_copy(
                wd.at[:, pl.ds(pl.multiple_of(b * wb, wb), wb)], block_slot(b), dsem.at[lax.rem(b, nslots)]
            )

        def q_copy(h):
            return pltpu.make_async_copy(
                wq.at[:, pl.ds(pl.multiple_of(h * qw, qw), qw)], qkvbuf.at[h, pl.ds(0, cb)], wsem.at[h]
            )

        kv_copies = [
            pltpu.make_async_copy(wk, qkvbuf.at[0, pl.ds(0, cb), pl.ds(0, lh * HD)], wsem.at[lh]),
            pltpu.make_async_copy(wv, qkvbuf.at[0, pl.ds(0, cb), pl.ds(lh * HD, lh * HD)], wsem.at[lh + 1]),
        ]

        def k_copy(p):
            return pltpu.make_async_copy(key_hbm.at[p], kbuf.at[p], ksem.at[p])

        def v_copy(p):
            slot = lax.rem(p, vslots)
            return pltpu.make_async_copy(val_hbm.at[p], vbuf.at[slot], vsem.at[slot])

        wo_copy = pltpu.make_async_copy(wo, wobuf, bigsem.at[0])
        wg_copy = pltpu.make_async_copy(wg, wgbuf, bigsem.at[1])
        wu_copy = pltpu.make_async_copy(wu, wubuf, bigsem.at[2])

        for h in range(lh):
            q_copy(h).start()

        @pl.loop(0, prompts)
        def _(p):
            k_copy(p).start()

        for p in range(vslots):
            v_copy(p).start()
        wo_copy.start()
        wg_copy.start()
        wu_copy.start()

        barrier = pltpu.get_barrier_semaphore()

        @pl.loop(1, n)
        def _(k):
            pl.semaphore_signal(barrier, inc=1, device_id={"pool": lax.rem(me + k, n)}, device_id_type=MESH)

        pl.semaphore_signal(barrier, inc=1, device_id={"heads": other}, device_id_type=MESH)

        def pool_copy(src, dst, ssem, rsem, d):
            return pltpu.make_async_remote_copy(
                src_ref=src, dst_ref=dst, send_sem=ssem.at[d], recv_sem=rsem.at[me],
                device_id={"pool": d}, device_id_type=MESH,
            )

        def wait_from(src, dst, ssem, rsem, s):
            pltpu.make_async_remote_copy(
                src_ref=src, dst_ref=dst, send_sem=ssem.at[s], recv_sem=rsem.at[s],
                device_id={"pool": s}, device_id_type=MESH,
            ).wait_recv()

        def peers(body):
            @pl.loop(1, n)
            def _(k):
                body(lax.rem(me + k, n))

        lane_row = lax.broadcasted_iota(jnp.int32, (1, HD), 1)
        hid = hidden[...].astype(F32)
        inv_rms = lax.rsqrt(jnp.sum(hid * hid, -1, keepdims=True) * (1.0 / d_model) + EPS)
        my_cols = hidden[:, pl.ds(pl.multiple_of(me * cb, cb), cb)].astype(F32)
        normed = (my_cols * inv_rms).astype(BF16)

        def put(h, c, value):
            for t in range(per_head):
                chunk[h * per_head + t, c] = value[t * ipd : (t + 1) * ipd]

        @pl.loop(0, lh)
        def _(h):
            q_copy(h).wait()
            res = jnp.dot(normed, qkvbuf[h, 0:cb, :], preferred_element_type=F32)
            for c in range(group):
                put(h, c, res[:, c * HD : (c + 1) * HD])

            @pl.when(h == 0)
            def _():
                for c in kv_copies:
                    c.start()

        for c in kv_copies:
            c.wait()
        res = jnp.dot(normed, qkvbuf[0, 0:cb, :], preferred_element_type=F32)
        for h in range(lh):
            put(h, group, res[:, h * HD : (h + 1) * HD])
            put(h, group + 1, res[:, (lh + h) * HD : (lh + h + 1) * HD])

        for b in range(min(nslots, nblocks)):
            down_copy(b).start()

        pl.semaphore_wait(barrier, n)
        peers(lambda d: pool_copy(chunk.at[d], chunk_in.at[me], s1, r1, d).start())

        inv_row = inv[...]

        cos_q, sin_q = rope_tables(qsel[...], inv_row, lane_row)
        tabs[0] = cos_q
        tabs[1] = sin_q

        @pl.loop(0, prompts)
        def _(p):
            k_copy(p).wait()
            ids = lax.dot_general(posx[p], sel[...], (((0,), (0,)), ((), ())), preferred_element_type=F32)
            cos_table, sin_table = rope_tables(ids, inv_row, lane_row)
            for h in range(lh):
                keys = kbuf[p, h].astype(F32)
                swapped = pltpu.roll(keys, HD // 2, 1)
                kbuf[p, h] = (keys * cos_table + swapped * sin_table).astype(BF16)

        total = chunk[me]

        def add_in(k, total):
            s = lax.rem(me + k, n)
            wait_from(chunk.at[s], chunk_in.at[s], s1, r1, s)
            return total + chunk_in[s]

        total = lax.fori_loop(1, n, add_in, total)
        first_prompt = lax.rem(me * ipd, prompts)
        if ipd % 8 == 0:
            first_prompt = pl.multiple_of(first_prompt, 8)
        cos_mine = tabs[0, pl.ds(first_prompt, ipd), :]
        sin_mine = tabs[1, pl.ds(first_prompt, ipd), :]
        for c in range(cols):
            value = total[c]
            if c <= group:
                value = value * cos_mine + pltpu.roll(value, HD // 2, 1) * sin_mine
            tr[:, c, :] = value
        for c in range(cols, 16):
            tr[:, c, :] = jnp.zeros((ipd, HD), F32)
        qg[me] = tr[...].astype(BF16)
        peers(lambda d: pool_copy(qg.at[me], qg.at[me], s2, r2, d).start())
        peers(lambda s: wait_from(qg.at[me], qg.at[s], s2, r2, s))

        slot_index = lax.broadcasted_iota(jnp.int32, (1, seq), 1) + me * seq

        @pl.loop(0, prompts)
        def _(p):
            v_copy(p).wait()
            slot = lax.rem(p, vslots)
            valid = slot_index < lens[p]
            for h in range(lh):
                it = h * prompts + p
                d = it // ipd
                i = lax.rem(it, ipd)
                queries = qg[d, i][0:group]
                scores = lax.dot_general(
                    queries, kbuf[p, h], (((1,), (1,)), ((), ())), preferred_element_type=F32
                ) * scale
                scores = jnp.where(valid, scores, -1e30)
                peak = jnp.max(scores, -1, keepdims=True)
                weights = jnp.where(valid, jnp.exp(scores - peak), 0.0)
                sums = jnp.sum(weights, -1, keepdims=True)
                acc[d, i] = jnp.dot(weights.astype(BF16), vbuf[slot, h], preferred_element_type=F32)
                ml[d] = jnp.where(lane_row == i, peak, jnp.where(lane_row == i + HD // 2, sums, ml[d]))

            @pl.when(p + vslots < prompts)
            def _():
                v_copy(p + vslots).start()

        def send_partial(d):
            pool_copy(acc.at[d], acc_in.at[me], s3, r3, d).start()
            pool_copy(ml.at[d], ml_in.at[me], s4, r4, d).start()

        peers(send_partial)

        own_scores = []
        for i in range(ipd):
            row = qg[me, i].astype(F32)
            own_scores.append(jnp.sum(row[0:group] * row[group : group + 1], -1, keepdims=True) * scale)

        def wait_partial(s):
            wait_from(acc.at[s], acc_in.at[s], s3, r3, s)
            wait_from(ml.at[s], ml_in.at[s], s4, r4, s)

        peers(wait_partial)
        acc_in[me] = acc[me]
        ml_in[me] = ml[me]

        top_all = lax.fori_loop(0, n, lambda s, t: jnp.maximum(t, ml_in[s]), jnp.full((group, HD), -1e30, F32))
        for i in range(ipd):
            top = jnp.maximum(top_all[:, i : i + 1], own_scores[i])
            own_weight = jnp.exp(own_scores[i] - top)
            own_value = qg[me, i].astype(F32)[group + 1 : group + 2]

            def merge(s, carry):
                den, num = carry
                tile = ml_in[s]
                factor = jnp.exp(tile[:, i : i + 1] - top)
                return den + tile[:, HD // 2 + i : HD // 2 + i + 1] * factor, num + acc_in[s, i] * factor

            den, num = lax.fori_loop(
                0, n, merge, (own_weight, own_weight * own_value), unroll=n <= 8
            )
            atf[i] = num / den
        for j in range(group):
            ats[:, j * HD : (j + 1) * HD] = atf[:, j, :].astype(BF16)
        atg[me] = ats[...]
        peers(lambda d: pool_copy(ats, atg.at[me], s5, r5, d).start())
        peers(lambda s: wait_from(ats, atg.at[s], s5, r5, s))

        wo_copy.wait()
        part[...] = jnp.zeros_like(part)

        @pl.loop(0, lh)
        def _(h):
            rows = atg[pl.ds(h * per_head, per_head)].astype(F32).reshape(prompts, qw).astype(BF16)
            part[...] += jnp.dot(rows, wobuf[pl.ds(pl.multiple_of(h * qw, qw), qw), :], preferred_element_type=F32)

        def partner_copy(src, dst, idx):
            return pltpu.make_async_remote_copy(
                src_ref=src, dst_ref=dst, send_sem=hs.at[idx], recv_sem=hr.at[idx],
                device_id={"heads": other}, device_id_type=MESH,
            )

        part_copy = partner_copy(part, part_in, 0)
        part_copy.start()
        part_copy.wait_recv()
        mid = (my_cols + (part[...] + part_in[...])).astype(BF16).astype(F32)
        midf[0] = mid[0:half_rows]
        midf[1] = mid[half_rows:]
        mid_send[...] = midf[hd].astype(BF16)
        mg[hd, me] = mid_send[...]
        peers(lambda d: pool_copy(mid_send, mg.at[hd, me], s6, r6, d).start())
        peers(lambda s: wait_from(mid_send, mg.at[hd, s], s6, r6, s))
        half_copy = partner_copy(mg.at[hd], mg.at[hd], 1)
        half_copy.start()
        pltpu.make_async_remote_copy(
            src_ref=mg.at[other], dst_ref=mg.at[other], send_sem=hs.at[1], recv_sem=hr.at[1],
            device_id={"heads": other}, device_id_type=MESH,
        ).wait_recv()

        def squares(s, total):
            x = mg[:, s].astype(F32).reshape(prompts, cb)
            return total + jnp.sum(x * x, -1, keepdims=True)

        sq = lax.fori_loop(0, n, squares, jnp.zeros((prompts, 1), F32))
        inv_mid = lax.rsqrt(sq * (1.0 / d_model) + EPS)
        wg_copy.wait()
        wu_copy.wait()

        def ff(s, carry):
            g, u = carry
            x = (mg[:, s].astype(F32).reshape(prompts, cb) * inv_mid).astype(BF16)
            rows = pl.ds(pl.multiple_of(s * cb, cb), cb)
            g = g + jnp.dot(x, wgbuf[rows, :], preferred_element_type=F32)
            u = u + jnp.dot(x, wubuf[rows, :], preferred_element_type=F32)
            return g, u

        zero = jnp.zeros((prompts, ffl), F32)
        gate, up = lax.fori_loop(0, n, ff, (zero, zero))
        ns[...] = (gate / (1.0 + jnp.exp(-gate)) * up).astype(BF16)

        per_block = wb // cb

        def dother_copy(d):
            return pltpu.make_async_remote_copy(
                src_ref=dpart.at[other, d], dst_ref=dother.at[d], send_sem=s7.at[d], recv_sem=r7.at[d],
                device_id={"heads": other}, device_id_type=MESH,
            )

        @pl.loop(0, nblocks)
        def _(b):
            down_copy(b).wait()
            slot = lax.rem(b, nslots)
            w = qkvbuf[slot, 0:ffl, :] if share else maybe_down[0][slot]
            res = jnp.dot(ns[...], w, preferred_element_type=F32)
            for t in range(per_block):
                d = b * per_block + t
                dpart[0, d] = res[0:half_rows, t * cb : (t + 1) * cb]
                dpart[1, d] = res[half_rows:, t * cb : (t + 1) * cb]
                dother_copy(d).start()

            @pl.when(b + nslots < nblocks)
            def _():
                down_copy(b + nslots).start()

        def reduce_and_send(d):
            dother_copy(d).wait_recv()
            ssum[d] = dpart[hd, d] + dother[d]
            pool_copy(ssum.at[d], rsum.at[me], s8, r8, d).start()

        peers(reduce_and_send)
        dother_copy(me).wait_recv()
        final = dpart[hd, me] + dother[me]

        def add_final(k, total):
            s = lax.rem(me + k, n)
            wait_from(ssum.at[s], rsum.at[s], s8, r8, s)
            return total + rsum[s]

        final = lax.fori_loop(1, n, add_final, final)
        yb[hd] = (midf[hd] + final).astype(BF16)
        y_copy = partner_copy(yb.at[hd], yb.at[hd], 2)
        y_copy.start()
        pltpu.make_async_remote_copy(
            src_ref=yb.at[other], dst_ref=yb.at[other], send_sem=hs.at[2], recv_sem=hr.at[2],
            device_id={"heads": other}, device_id_type=MESH,
        ).wait_recv()
        out_ref[...] = yb[...].astype(F32).reshape(prompts, cb).astype(BF16)

        def drain(d):
            pool_copy(chunk.at[d], chunk_in.at[me], s1, r1, d).wait_send()
            pool_copy(qg.at[me], qg.at[me], s2, r2, d).wait_send()
            pool_copy(acc.at[d], acc_in.at[me], s3, r3, d).wait_send()
            pool_copy(ml.at[d], ml_in.at[me], s4, r4, d).wait_send()
            pool_copy(ats, atg.at[me], s5, r5, d).wait_send()
            pool_copy(mid_send, mg.at[hd, me], s6, r6, d).wait_send()
            pool_copy(ssum.at[d], rsum.at[me], s8, r8, d).wait_send()

        peers(drain)

        @pl.loop(0, n)
        def _(d):
            dother_copy(d).wait_send()

        part_copy.wait_send()
        half_copy.wait_send()
        y_copy.wait_send()

    return kernel


def per_device(
    n, hidden_in, key_cache, value_cache, positions, query_pos, lengths,
    query_weight, key_weight, value_weight, out_weight, gate_weight, up_weight, down_weight,
):
    prompts, d_model = hidden_in.shape
    lh, seq = key_cache.shape[1:3]
    cb = d_model // n
    ffl = gate_weight.shape[1]
    group = query_weight.shape[1] // key_weight.shape[1]
    qw = group * HD
    wb = max(cb, qw)
    nblocks = d_model // wb
    nslots = min(lh, nblocks)
    share = ffl % 16 == 0 and ffl <= cb and wb == qw
    vslots = 3
    items = prompts * lh
    ipd = items // n

    column = jnp.arange(HD) % (HD // 2)
    inverse = jnp.exp(column.astype(F32) * (-2.0 * math.log(THETA) / HD))[None]
    first_end = HD // 8
    second_end = first_end + 3 * HD // 16
    which = jnp.where(column < first_end, 0, jnp.where(column < second_end, 1, 2))
    hit = (which[None] == jnp.arange(3)[:, None]).astype(F32)
    pad = jnp.zeros((2, HD), F32)
    sel = jnp.concatenate([64.0 * hit, hit, pad], 0).astype(BF16)
    spread = jnp.transpose(positions, (1, 0, 2))
    posx = jnp.concatenate(
        [spread // 64, spread % 64, jnp.zeros((prompts, 2, seq), jnp.int32)], 1
    ).astype(BF16)
    qpos = query_pos.astype(F32)
    qsel = jnp.where(
        column < first_end, qpos[0][:, None], jnp.where(column < second_end, qpos[1][:, None], qpos[2][:, None])
    )

    kernel = make_kernel(n, prompts, lh, seq, d_model, ffl, group, wb, nslots, vslots, share)
    half = prompts // 2
    vm = pltpu.VMEM
    dma = pltpu.SemaphoreType.DMA
    scratch = [
        vm((prompts, lh, seq, HD), BF16),
        vm((vslots, lh, seq, HD), BF16),
        vm((lh, cb, qw), BF16),
        vm(out_weight.shape, BF16),
        vm(gate_weight.shape, BF16),
        vm(up_weight.shape, BF16),
        vm((n, group + 2, ipd, HD), F32),
        vm((n, group + 2, ipd, HD), F32),
        vm((ipd, 16, HD), F32),
        vm((n, ipd, 16, HD), BF16),
        vm((n, ipd, group, HD), F32),
        vm((n, ipd, group, HD), F32),
        vm((n, group, HD), F32),
        vm((n, group, HD), F32),
        vm((ipd, group, HD), F32),
        vm((ipd, qw), BF16),
        vm((n, ipd, qw), BF16),
        vm((prompts, cb), F32),
        vm((prompts, cb), F32),
        vm((2, half, cb), F32),
        vm((half, cb), BF16),
        vm((2, n, half, cb), BF16),
        vm((prompts, ffl), BF16),
        vm((2, n, half, cb), F32),
        vm((n, half, cb), F32),
        vm((n, half, cb), F32),
        vm((n, half, cb), F32),
        vm((2, half, cb), BF16),
        vm((2, prompts, HD), F32),
        dma((lh + 2,)),
        dma((prompts,)),
        dma((vslots,)),
        dma((3,)),
        dma((nslots,)),
    ] + [dma((n,)) for _ in range(16)] + [dma((3,)), dma((3,))]
    if not share:
        scratch.append(vm((nslots, ffl, wb), BF16))
    in_vmem = pl.BlockSpec(memory_space=pltpu.VMEM)
    in_any = pl.BlockSpec(memory_space=pl.ANY)
    return pl.pallas_call(
        kernel,
        out_shape=jax.ShapeDtypeStruct((prompts, cb), BF16),
        in_specs=[in_vmem] * 5 + [pl.BlockSpec(memory_space=pltpu.SMEM)] + [in_any] * 9,
        out_specs=in_vmem,
        scratch_shapes=scratch,
        compiler_params=pltpu.CompilerParams(
            collective_id=0, has_side_effects=True, vmem_limit_bytes=67043328
        ),
    )(
        hidden_in, posx, sel, qsel, inverse, lengths, key_cache, value_cache,
        query_weight, key_weight, value_weight, out_weight, gate_weight, up_weight, down_weight,
    )


def solution(mesh):
    in_specs = (
        P("groups", None),
        P("groups", "heads", "pool", None),
        P("groups", "heads", "pool", None),
        P(None, "groups", "pool"),
        P(None, "groups"),
        P("groups"),
        P("pool", "heads"),
        P("pool", "heads"),
        P("pool", "heads"),
        P("heads", "pool"),
        P(None, ("pool", "heads")),
        P(None, ("pool", "heads")),
        P(("pool", "heads"), None),
    )
    return jax.shard_map(
        functools.partial(per_device, mesh.shape["pool"]),
        mesh=mesh,
        in_specs=in_specs,
        out_specs=P("groups", "pool"),
        check_vma=False,
    )
```

```python
import functools
import math

import jax
import jax.numpy as jnp
from jax import lax
from jax.experimental import pallas as pl
from jax.experimental.pallas import tpu as pltpu
from jax.sharding import PartitionSpec as P

HD = 128
EPS = 1e-06
THETA = 1000000.0
MESH = pl.DeviceIdType.MESH
F32 = jnp.float32
BF16 = jnp.bfloat16

TURN_A = 6.28125
TURN_B = round((2 * math.pi - TURN_A) * 2**20) / 2**20
TURN_C = 2 * math.pi - TURN_A - TURN_B
SINE = [(-1) ** i / math.factorial(2 * i + 1) for i in range(7)]


def rope_tables(ids, inverse, lane):
    angle = ids * inverse
    upper = lane >= HD // 2
    quarter = jnp.where(upper, 0.25, 0.0).astype(F32)
    turns = jnp.floor(angle * (1.0 / (2 * math.pi)) - quarter + 0.5)
    rest = angle - turns * TURN_A
    rest = rest - turns * TURN_B
    rest = rest - turns * TURN_C
    half = (rest - quarter * (2 * math.pi)) * 0.5
    square = half * half
    poly = jnp.full_like(square, SINE[6])
    for i in range(5, -1, -1):
        poly = poly * square + SINE[i]
    sine = poly * half
    table = 1.0 - 2.0 * sine * sine
    swapped = pltpu.roll(table, HD // 2, 1)
    cos_table = jnp.where(upper, swapped, table)
    sin_table = jnp.where(upper, table, -swapped)
    return cos_table, sin_table


def make_kernel(n, prompts, lh, seq, d_model, ffl, group, wb, nslots, vslots, share):
    cb = d_model // n
    items = prompts * lh
    ipd = items // n
    per_head = prompts // ipd
    qw = group * HD
    cols = group + 2
    half_rows = prompts // 2
    nblocks = d_model // wb
    scale = HD ** (-0.5)

    def kernel(
        hidden, posx, sel, qsel, inv, lens, key_hbm, val_hbm, wq, wk, wv, wo, wg, wu, wd,
        out_ref,
        kbuf, vbuf, qkvbuf, wobuf, wgbuf, wubuf, chunk, chunk_in, tr, qg, acc, acc_in, ml, ml_in,
        atf, ats, atg, part, part_in, midf, mid_send, mg, ns, dpart, dother, ssum, rsum, yb, tabs,
        wsem, ksem, vsem, bigsem, dsem,
        s1, r1, s2, r2, s3, r3, s4, r4, s5, r5, s6, r6, s7, r7, s8, r8, hs, hr,
        *maybe_down,
    ):
        me = lax.axis_index("pool")
        hd = lax.axis_index("heads")
        other = 1 - hd

        def block_slot(b):
            buf = qkvbuf if share else maybe_down[0]
            slot = lax.rem(b, nslots)
            return buf.at[slot, pl.ds(0, ffl)] if share else buf.at[slot]

        def down_copy(b):
            return pltpu.make_async_copy(
                wd.at[:, pl.ds(pl.multiple_of(b * wb, wb), wb)], block_slot(b), dsem.at[lax.rem(b, nslots)]
            )

        def q_copy(h):
            return pltpu.make_async_copy(
                wq.at[:, pl.ds(pl.multiple_of(h * qw, qw), qw)], qkvbuf.at[h, pl.ds(0, cb)], wsem.at[h]
            )

        kv_copies = [
            pltpu.make_async_copy(wk, qkvbuf.at[0, pl.ds(0, cb), pl.ds(0, lh * HD)], wsem.at[lh]),
            pltpu.make_async_copy(wv, qkvbuf.at[0, pl.ds(0, cb), pl.ds(lh * HD, lh * HD)], wsem.at[lh + 1]),
        ]

        def k_copy(p):
            return pltpu.make_async_copy(key_hbm.at[p], kbuf.at[p], ksem.at[p])

        def v_copy(p):
            slot = lax.rem(p, vslots)
            return pltpu.make_async_copy(val_hbm.at[p], vbuf.at[slot], vsem.at[slot])

        wo_copy = pltpu.make_async_copy(wo, wobuf, bigsem.at[0])
        wg_copy = pltpu.make_async_copy(wg, wgbuf, bigsem.at[1])
        wu_copy = pltpu.make_async_copy(wu, wubuf, bigsem.at[2])

        for h in range(lh):
            q_copy(h).start()

        @pl.loop(0, prompts)
        def _(p):
            k_copy(p).start()

        for p in range(vslots):
            v_copy(p).start()
        wo_copy.start()
        wg_copy.start()
        wu_copy.start()

        barrier = pltpu.get_barrier_semaphore()

        @pl.loop(1, n)
        def _(k):
            pl.semaphore_signal(barrier, inc=1, device_id={"pool": lax.rem(me + k, n)}, device_id_type=MESH)

        pl.semaphore_signal(barrier, inc=1, device_id={"heads": other}, device_id_type=MESH)

        def pool_copy(src, dst, ssem, rsem, d):
            return pltpu.make_async_remote_copy(
                src_ref=src, dst_ref=dst, send_sem=ssem.at[d], recv_sem=rsem.at[me],
                device_id={"pool": d}, device_id_type=MESH,
            )

        def wait_from(src, dst, ssem, rsem, s):
            pltpu.make_async_remote_copy(
                src_ref=src, dst_ref=dst, send_sem=ssem.at[s], recv_sem=rsem.at[s],
                device_id={"pool": s}, device_id_type=MESH,
            ).wait_recv()

        def peers(body):
            @pl.loop(1, n)
            def _(k):
                body(lax.rem(me + k, n))

        lane_row = lax.broadcasted_iota(jnp.int32, (1, HD), 1)
        hid = hidden[...].astype(F32)
        inv_rms = lax.rsqrt(jnp.sum(hid * hid, -1, keepdims=True) * (1.0 / d_model) + EPS)
        my_cols = hidden[:, pl.ds(pl.multiple_of(me * cb, cb), cb)].astype(F32)
        normed = (my_cols * inv_rms).astype(BF16)

        def put(h, c, value):
            for t in range(per_head):
                chunk[h * per_head + t, c] = value[t * ipd : (t + 1) * ipd]

        @pl.loop(0, lh)
        def _(h):
            q_copy(h).wait()
            res = jnp.dot(normed, qkvbuf[h, 0:cb, :], preferred_element_type=F32)
            for c in range(group):
                put(h, c, res[:, c * HD : (c + 1) * HD])

            @pl.when(h == 0)
            def _():
                for c in kv_copies:
                    c.start()

        for c in kv_copies:
            c.wait()
        res = jnp.dot(normed, qkvbuf[0, 0:cb, :], preferred_element_type=F32)
        for h in range(lh):
            put(h, group, res[:, h * HD : (h + 1) * HD])
            put(h, group + 1, res[:, (lh + h) * HD : (lh + h + 1) * HD])

        for b in range(min(nslots, nblocks)):
            down_copy(b).start()

        pl.semaphore_wait(barrier, n)
        peers(lambda d: pool_copy(chunk.at[d], chunk_in.at[me], s1, r1, d).start())

        inv_row = inv[...]

        cos_q, sin_q = rope_tables(qsel[...], inv_row, lane_row)
        tabs[0] = cos_q
        tabs[1] = sin_q

        @pl.loop(0, prompts)
        def _(p):
            k_copy(p).wait()
            ids = lax.dot_general(posx[p], sel[...], (((0,), (0,)), ((), ())), preferred_element_type=F32)
            cos_table, sin_table = rope_tables(ids, inv_row, lane_row)
            for h in range(lh):
                keys = kbuf[p, h].astype(F32)
                swapped = pltpu.roll(keys, HD // 2, 1)
                kbuf[p, h] = (keys * cos_table + swapped * sin_table).astype(BF16)

        total = chunk[me]

        def add_in(k, total):
            s = lax.rem(me + k, n)
            wait_from(chunk.at[s], chunk_in.at[s], s1, r1, s)
            return total + chunk_in[s]

        total = lax.fori_loop(1, n, add_in, total)
        first_prompt = lax.rem(me * ipd, prompts)
        if ipd % 8 == 0:
            first_prompt = pl.multiple_of(first_prompt, 8)
        cos_mine = tabs[0, pl.ds(first_prompt, ipd), :]
        sin_mine = tabs[1, pl.ds(first_prompt, ipd), :]
        for c in range(cols):
            value = total[c]
            if c <= group:
                value = value * cos_mine + pltpu.roll(value, HD // 2, 1) * sin_mine
            tr[:, c, :] = value
        for c in range(cols, 16):
            tr[:, c, :] = jnp.zeros((ipd, HD), F32)
        qg[me] = tr[...].astype(BF16)
        peers(lambda d: pool_copy(qg.at[me], qg.at[me], s2, r2, d).start())
        peers(lambda s: wait_from(qg.at[me], qg.at[s], s2, r2, s))

        slot_index = lax.broadcasted_iota(jnp.int32, (1, seq), 1) + me * seq

        @pl.loop(0, prompts)
        def _(p):
            v_copy(p).wait()
            slot = lax.rem(p, vslots)
            valid = slot_index < lens[p]
            for h in range(lh):
                it = h * prompts + p
                d = it // ipd
                i = lax.rem(it, ipd)
                queries = qg[d, i][0:group]
                scores = lax.dot_general(
                    queries, kbuf[p, h], (((1,), (1,)), ((), ())), preferred_element_type=F32
                ) * scale
                scores = jnp.where(valid, scores, -1e30)
                peak = jnp.max(scores, -1, keepdims=True)
                weights = jnp.where(valid, jnp.exp(scores - peak), 0.0)
                sums = jnp.sum(weights, -1, keepdims=True)
                acc[d, i] = jnp.dot(weights.astype(BF16), vbuf[slot, h], preferred_element_type=F32)
                ml[d] = jnp.where(lane_row == i, peak, jnp.where(lane_row == i + HD // 2, sums, ml[d]))

            @pl.when(p + vslots < prompts)
            def _():
                v_copy(p + vslots).start()

        def send_partial(d):
            pool_copy(acc.at[d], acc_in.at[me], s3, r3, d).start()
            pool_copy(ml.at[d], ml_in.at[me], s4, r4, d).start()

        peers(send_partial)

        own_scores = []
        for i in range(ipd):
            row = qg[me, i].astype(F32)
            own_scores.append(jnp.sum(row[0:group] * row[group : group + 1], -1, keepdims=True) * scale)

        def wait_partial(s):
            wait_from(acc.at[s], acc_in.at[s], s3, r3, s)
            wait_from(ml.at[s], ml_in.at[s], s4, r4, s)

        peers(wait_partial)
        acc_in[me] = acc[me]
        ml_in[me] = ml[me]

        top_all = lax.fori_loop(0, n, lambda s, t: jnp.maximum(t, ml_in[s]), jnp.full((group, HD), -1e30, F32))
        for i in range(ipd):
            top = jnp.maximum(top_all[:, i : i + 1], own_scores[i])
            own_weight = jnp.exp(own_scores[i] - top)
            own_value = qg[me, i].astype(F32)[group + 1 : group + 2]

            def merge(s, carry):
                den, num = carry
                tile = ml_in[s]
                factor = jnp.exp(tile[:, i : i + 1] - top)
                return den + tile[:, HD // 2 + i : HD // 2 + i + 1] * factor, num + acc_in[s, i] * factor

            den, num = lax.fori_loop(
                0, n, merge, (own_weight, own_weight * own_value), unroll=n <= 8
            )
            atf[i] = num / den
        for j in range(group):
            ats[:, j * HD : (j + 1) * HD] = atf[:, j, :].astype(BF16)
        atg[me] = ats[...]
        peers(lambda d: pool_copy(ats, atg.at[me], s5, r5, d).start())
        peers(lambda s: wait_from(ats, atg.at[s], s5, r5, s))

        wo_copy.wait()
        part[...] = jnp.zeros_like(part)

        @pl.loop(0, lh)
        def _(h):
            rows = atg[pl.ds(h * per_head, per_head)].astype(F32).reshape(prompts, qw).astype(BF16)
            part[...] += jnp.dot(rows, wobuf[pl.ds(pl.multiple_of(h * qw, qw), qw), :], preferred_element_type=F32)

        def partner_copy(src, dst, idx):
            return pltpu.make_async_remote_copy(
                src_ref=src, dst_ref=dst, send_sem=hs.at[idx], recv_sem=hr.at[idx],
                device_id={"heads": other}, device_id_type=MESH,
            )

        part_copy = partner_copy(part, part_in, 0)
        part_copy.start()
        part_copy.wait_recv()
        mid = (my_cols + (part[...] + part_in[...])).astype(BF16).astype(F32)
        midf[0] = mid[0:half_rows]
        midf[1] = mid[half_rows:]
        mid_send[...] = midf[hd].astype(BF16)
        mg[hd, me] = mid_send[...]
        peers(lambda d: pool_copy(mid_send, mg.at[hd, me], s6, r6, d).start())
        peers(lambda s: wait_from(mid_send, mg.at[hd, s], s6, r6, s))
        half_copy = partner_copy(mg.at[hd], mg.at[hd], 1)
        half_copy.start()
        pltpu.make_async_remote_copy(
            src_ref=mg.at[other], dst_ref=mg.at[other], send_sem=hs.at[1], recv_sem=hr.at[1],
            device_id={"heads": other}, device_id_type=MESH,
        ).wait_recv()

        def squares(s, total):
            x = mg[:, s].astype(F32).reshape(prompts, cb)
            return total + jnp.sum(x * x, -1, keepdims=True)

        sq = lax.fori_loop(0, n, squares, jnp.zeros((prompts, 1), F32))
        inv_mid = lax.rsqrt(sq * (1.0 / d_model) + EPS)
        wg_copy.wait()
        wu_copy.wait()

        def ff(s, carry):
            g, u = carry
            x = (mg[:, s].astype(F32).reshape(prompts, cb) * inv_mid).astype(BF16)
            rows = pl.ds(pl.multiple_of(s * cb, cb), cb)
            nt = (((1,), (1,)), ((), ()))
            g = g + lax.dot_general(x, wgbuf[:, rows], nt, preferred_element_type=F32)
            u = u + lax.dot_general(x, wubuf[:, rows], nt, preferred_element_type=F32)
            return g, u

        zero = jnp.zeros((prompts, ffl), F32)
        gate, up = lax.fori_loop(0, n, ff, (zero, zero))
        ns[...] = (gate / (1.0 + jnp.exp(-gate)) * up).astype(BF16)

        per_block = wb // cb

        def dother_copy(d):
            return pltpu.make_async_remote_copy(
                src_ref=dpart.at[other, d], dst_ref=dother.at[d], send_sem=s7.at[d], recv_sem=r7.at[d],
                device_id={"heads": other}, device_id_type=MESH,
            )

        @pl.loop(0, nblocks)
        def _(b):
            down_copy(b).wait()
            slot = lax.rem(b, nslots)
            w = qkvbuf[slot, 0:ffl, :] if share else maybe_down[0][slot]
            res = jnp.dot(ns[...], w, preferred_element_type=F32)
            for t in range(per_block):
                d = b * per_block + t
                dpart[0, d] = res[0:half_rows, t * cb : (t + 1) * cb]
                dpart[1, d] = res[half_rows:, t * cb : (t + 1) * cb]
                dother_copy(d).start()

            @pl.when(b + nslots < nblocks)
            def _():
                down_copy(b + nslots).start()

        def reduce_and_send(d):
            dother_copy(d).wait_recv()
            ssum[d] = dpart[hd, d] + dother[d]
            pool_copy(ssum.at[d], rsum.at[me], s8, r8, d).start()

        peers(reduce_and_send)
        dother_copy(me).wait_recv()
        final = dpart[hd, me] + dother[me]

        def add_final(k, total):
            s = lax.rem(me + k, n)
            wait_from(ssum.at[s], rsum.at[s], s8, r8, s)
            return total + rsum[s]

        final = lax.fori_loop(1, n, add_final, final)
        yb[hd] = (midf[hd] + final).astype(BF16)
        y_copy = partner_copy(yb.at[hd], yb.at[hd], 2)
        y_copy.start()
        pltpu.make_async_remote_copy(
            src_ref=yb.at[other], dst_ref=yb.at[other], send_sem=hs.at[2], recv_sem=hr.at[2],
            device_id={"heads": other}, device_id_type=MESH,
        ).wait_recv()
        out_ref[...] = yb[...].astype(F32).reshape(prompts, cb).astype(BF16)

        def drain(d):
            pool_copy(chunk.at[d], chunk_in.at[me], s1, r1, d).wait_send()
            pool_copy(qg.at[me], qg.at[me], s2, r2, d).wait_send()
            pool_copy(acc.at[d], acc_in.at[me], s3, r3, d).wait_send()
            pool_copy(ml.at[d], ml_in.at[me], s4, r4, d).wait_send()
            pool_copy(ats, atg.at[me], s5, r5, d).wait_send()
            pool_copy(mid_send, mg.at[hd, me], s6, r6, d).wait_send()
            pool_copy(ssum.at[d], rsum.at[me], s8, r8, d).wait_send()

        peers(drain)

        @pl.loop(0, n)
        def _(d):
            dother_copy(d).wait_send()

        part_copy.wait_send()
        half_copy.wait_send()
        y_copy.wait_send()

    return kernel


def per_device(
    n, hidden_in, key_cache, value_cache, positions, query_pos, lengths,
    query_weight, key_weight, value_weight, out_weight, gate_weight, up_weight, down_weight,
):
    prompts, d_model = hidden_in.shape
    lh, seq = key_cache.shape[1:3]
    cb = d_model // n
    ffl = gate_weight.shape[1]
    group = query_weight.shape[1] // key_weight.shape[1]
    qw = group * HD
    wb = max(cb, qw)
    nblocks = d_model // wb
    nslots = min(lh, nblocks)
    share = ffl % 16 == 0 and ffl <= cb and wb == qw
    vslots = 3
    items = prompts * lh
    ipd = items // n

    column = jnp.arange(HD) % (HD // 2)
    inverse = jnp.exp(column.astype(F32) * (-2.0 * math.log(THETA) / HD))[None]
    first_end = HD // 8
    second_end = first_end + 3 * HD // 16
    which = jnp.where(column < first_end, 0, jnp.where(column < second_end, 1, 2))
    hit = (which[None] == jnp.arange(3)[:, None]).astype(F32)
    pad = jnp.zeros((2, HD), F32)
    sel = jnp.concatenate([64.0 * hit, hit, pad], 0).astype(BF16)
    spread = jnp.transpose(positions, (1, 0, 2))
    posx = jnp.concatenate(
        [spread // 64, spread % 64, jnp.zeros((prompts, 2, seq), jnp.int32)], 1
    ).astype(BF16)
    qpos = query_pos.astype(F32)
    qsel = jnp.where(
        column < first_end, qpos[0][:, None], jnp.where(column < second_end, qpos[1][:, None], qpos[2][:, None])
    )

    kernel = make_kernel(n, prompts, lh, seq, d_model, ffl, group, wb, nslots, vslots, share)
    half = prompts // 2
    vm = pltpu.VMEM
    dma = pltpu.SemaphoreType.DMA
    scratch = [
        vm((prompts, lh, seq, HD), BF16),
        vm((vslots, lh, seq, HD), BF16),
        vm((lh, cb, qw), BF16),
        vm(out_weight.shape, BF16),
        vm((ffl, d_model), BF16),
        vm((ffl, d_model), BF16),
        vm((n, group + 2, ipd, HD), F32),
        vm((n, group + 2, ipd, HD), F32),
        vm((ipd, 16, HD), F32),
        vm((n, ipd, 16, HD), BF16),
        vm((n, ipd, group, HD), F32),
        vm((n, ipd, group, HD), F32),
        vm((n, group, HD), F32),
        vm((n, group, HD), F32),
        vm((ipd, group, HD), F32),
        vm((ipd, qw), BF16),
        vm((n, ipd, qw), BF16),
        vm((prompts, cb), F32),
        vm((prompts, cb), F32),
        vm((2, half, cb), F32),
        vm((half, cb), BF16),
        vm((2, n, half, cb), BF16),
        vm((prompts, ffl), BF16),
        vm((2, n, half, cb), F32),
        vm((n, half, cb), F32),
        vm((n, half, cb), F32),
        vm((n, half, cb), F32),
        vm((2, half, cb), BF16),
        vm((2, prompts, HD), F32),
        dma((lh + 2,)),
        dma((prompts,)),
        dma((vslots,)),
        dma((3,)),
        dma((nslots,)),
    ] + [dma((n,)) for _ in range(16)] + [dma((3,)), dma((3,))]
    if not share:
        scratch.append(vm((nslots, ffl, wb), BF16))
    in_vmem = pl.BlockSpec(memory_space=pltpu.VMEM)
    in_any = pl.BlockSpec(memory_space=pl.ANY)
    return pl.pallas_call(
        kernel,
        out_shape=jax.ShapeDtypeStruct((prompts, cb), BF16),
        in_specs=[in_vmem] * 5 + [pl.BlockSpec(memory_space=pltpu.SMEM)] + [in_any] * 9,
        out_specs=in_vmem,
        scratch_shapes=scratch,
        compiler_params=pltpu.CompilerParams(
            collective_id=0, has_side_effects=True, vmem_limit_bytes=67043328
        ),
    )(
        hidden_in, posx, sel, qsel, inverse, lengths, key_cache, value_cache,
        query_weight, key_weight, value_weight, out_weight, gate_weight.T, up_weight.T, down_weight,
    )


def solution(mesh):
    in_specs = (
        P("groups", None),
        P("groups", "heads", "pool", None),
        P("groups", "heads", "pool", None),
        P(None, "groups", "pool"),
        P(None, "groups"),
        P("groups"),
        P("pool", "heads"),
        P("pool", "heads"),
        P("pool", "heads"),
        P("heads", "pool"),
        P(None, ("pool", "heads")),
        P(None, ("pool", "heads")),
        P(("pool", "heads"), None),
    )
    return jax.shard_map(
        functools.partial(per_device, mesh.shape["pool"]),
        mesh=mesh,
        in_specs=in_specs,
        out_specs=P("groups", "pool"),
        check_vma=False,
    )
```

```python
import functools
import math

import jax
import jax.numpy as jnp
import numpy as np
from jax import lax
from jax.experimental import pallas as pl
from jax.experimental.pallas import tpu as pltpu
from jax.sharding import PartitionSpec as P

HD = 128
EPS = 1e-06
THETA = 1000000.0
MESH = pl.DeviceIdType.MESH
F32 = jnp.float32
BF16 = jnp.bfloat16

TURN_A = 6.28125
TURN_B = round((2 * math.pi - TURN_A) * 2**20) / 2**20
TURN_C = 2 * math.pi - TURN_A - TURN_B
SINE = [(-1) ** i / math.factorial(2 * i + 1) for i in range(7)]


def rope_tables(ids, inverse, lane):
    angle = ids * inverse
    upper = lane >= HD // 2
    quarter = jnp.where(upper, 0.25, 0.0).astype(F32)
    turns = jnp.floor(angle * (1.0 / (2 * math.pi)) - quarter + 0.5)
    rest = angle - turns * TURN_A
    rest = rest - turns * TURN_B
    rest = rest - turns * TURN_C
    half = (rest - quarter * (2 * math.pi)) * 0.5
    square = half * half
    poly = jnp.full_like(square, SINE[6])
    for i in range(5, -1, -1):
        poly = poly * square + SINE[i]
    sine = poly * half
    table = 1.0 - 2.0 * sine * sine
    swapped = pltpu.roll(table, HD // 2, 1)
    cos_table = jnp.where(upper, swapped, table)
    sin_table = jnp.where(upper, table, -swapped)
    return cos_table, sin_table


def make_kernel(n, prompts, lh, seq, d_model, ffl, group, wb, nslots, vslots, share):
    cb = d_model // n
    items = prompts * lh
    ipd = items // n
    per_head = prompts // ipd
    qw = group * HD
    cols = group + 2
    half_rows = prompts // 2
    nblocks = d_model // wb
    scale = HD ** (-0.5)

    def kernel(
        hidden, pos, qpos, sel, inv, lens, key_hbm, val_hbm, wq, wk, wv, wo, wg, wu, wd,
        out_ref,
        kbuf, vbuf, qkvbuf, wobuf, wgbuf, wubuf, chunk, chunk_in, tr, qg, acc, acc_in, ml, ml_in,
        atf, ats, atg, part, part_in, midf, mid_send, mg, ns, dpart, dother, ssum, rsum, yb, tabs,
        wsem, ksem, vsem, bigsem, dsem,
        s1, r1, s2, r2, s3, r3, s4, r4, s5, r5, s6, r6, s7, r7, s8, r8, hs, hr,
        *maybe_down,
    ):
        me = lax.axis_index("pool")
        hd = lax.axis_index("heads")
        other = 1 - hd

        def block_slot(b):
            buf = qkvbuf if share else maybe_down[0]
            slot = lax.rem(b, nslots)
            return buf.at[slot, pl.ds(0, ffl)] if share else buf.at[slot]

        def down_copy(b):
            return pltpu.make_async_copy(
                wd.at[:, pl.ds(pl.multiple_of(b * wb, wb), wb)], block_slot(b), dsem.at[lax.rem(b, nslots)]
            )

        def q_copy(h):
            return pltpu.make_async_copy(
                wq.at[:, pl.ds(pl.multiple_of(h * qw, qw), qw)], qkvbuf.at[h, pl.ds(0, cb)], wsem.at[h]
            )

        kv_copies = [
            pltpu.make_async_copy(wk, qkvbuf.at[0, pl.ds(0, cb), pl.ds(0, lh * HD)], wsem.at[lh]),
            pltpu.make_async_copy(wv, qkvbuf.at[0, pl.ds(0, cb), pl.ds(lh * HD, lh * HD)], wsem.at[lh + 1]),
        ]

        def k_copy(p):
            return pltpu.make_async_copy(key_hbm.at[p], kbuf.at[p], ksem.at[p])

        def v_copy(k):
            d = lax.rem(me + k, n)
            slot = lax.rem(k, vslots)
            first = pl.multiple_of(lax.rem(d, per_head) * ipd, ipd)
            return pltpu.make_async_copy(
                val_hbm.at[pl.ds(first, ipd), d // per_head], vbuf.at[slot], vsem.at[slot]
            )

        wo_copy = pltpu.make_async_copy(wo, wobuf, bigsem.at[0])
        wg_copy = pltpu.make_async_copy(wg, wgbuf, bigsem.at[1])
        wu_copy = pltpu.make_async_copy(wu, wubuf, bigsem.at[2])

        for h in range(lh):
            q_copy(h).start()

        @pl.loop(0, prompts)
        def _(p):
            k_copy(p).start()

        for k in range(1, vslots + 1):
            v_copy(k).start()
        wo_copy.start()
        wg_copy.start()
        wu_copy.start()

        barrier = pltpu.get_barrier_semaphore()

        @pl.loop(1, n)
        def _(k):
            pl.semaphore_signal(barrier, inc=1, device_id={"pool": lax.rem(me + k, n)}, device_id_type=MESH)

        pl.semaphore_signal(barrier, inc=1, device_id={"heads": other}, device_id_type=MESH)

        def pool_copy(src, dst, ssem, rsem, d):
            return pltpu.make_async_remote_copy(
                src_ref=src, dst_ref=dst, send_sem=ssem.at[d], recv_sem=rsem.at[me],
                device_id={"pool": d}, device_id_type=MESH,
            )

        def wait_from(src, dst, ssem, rsem, s):
            pltpu.make_async_remote_copy(
                src_ref=src, dst_ref=dst, send_sem=ssem.at[s], recv_sem=rsem.at[s],
                device_id={"pool": s}, device_id_type=MESH,
            ).wait_recv()

        def peers(body):
            @pl.loop(1, n)
            def _(k):
                body(lax.rem(me + k, n))

        lane_row = lax.broadcasted_iota(jnp.int32, (1, HD), 1)
        hid = hidden[...].astype(F32)
        inv_rms = lax.rsqrt(jnp.sum(hid * hid, -1, keepdims=True) * (1.0 / d_model) + EPS)
        my_cols = hidden[:, pl.ds(pl.multiple_of(me * cb, cb), cb)].astype(F32)
        normed = (my_cols * inv_rms).astype(BF16)

        def put(h, c, value):
            for t in range(per_head):
                chunk[h * per_head + t, c] = value[t * ipd : (t + 1) * ipd]

        @pl.loop(0, lh)
        def _(h):
            q_copy(h).wait()
            res = jnp.dot(normed, qkvbuf[h, 0:cb, :], preferred_element_type=F32)
            for c in range(group):
                put(h, c, res[:, c * HD : (c + 1) * HD])

            @pl.when(h == 0)
            def _():
                for c in kv_copies:
                    c.start()

        for c in kv_copies:
            c.wait()
        res = jnp.dot(normed, qkvbuf[0, 0:cb, :], preferred_element_type=F32)
        for h in range(lh):
            put(h, group, res[:, h * HD : (h + 1) * HD])
            put(h, group + 1, res[:, (lh + h) * HD : (lh + h + 1) * HD])

        for b in range(min(nslots, nblocks)):
            down_copy(b).start()

        pl.semaphore_wait(barrier, n)
        peers(lambda d: pool_copy(chunk.at[d], chunk_in.at[me], s1, r1, d).start())

        inv_row = inv[...]

        def split(ids):
            high = jnp.floor(ids * (1.0 / 64.0))
            pad = jnp.zeros((2, ids.shape[1]), F32)
            return jnp.concatenate([high, ids - 64.0 * high, pad], 0).astype(BF16)

        def pick(ids):
            return lax.dot_general(split(ids), sel[...], (((0,), (0,)), ((), ())), preferred_element_type=F32)

        cos_q, sin_q = rope_tables(pick(qpos[...].astype(F32)), inv_row, lane_row)
        tabs[0] = cos_q
        tabs[1] = sin_q

        def rotate_prompt(p):
            k_copy(p).wait()
            ids = pick(pos[:, p, :].astype(F32))
            cos_table, sin_table = rope_tables(ids, inv_row, lane_row)
            for h in range(lh):
                keys = kbuf[p, h].astype(F32)
                swapped = pltpu.roll(keys, HD // 2, 1)
                kbuf[p, h] = (keys * cos_table + swapped * sin_table).astype(BF16)

        pl.loop(0, prompts // 2)(rotate_prompt)

        total = chunk[me]

        def add_in(k, total):
            s = lax.rem(me + k, n)
            wait_from(chunk.at[s], chunk_in.at[s], s1, r1, s)
            return total + chunk_in[s]

        total = lax.fori_loop(1, n, add_in, total)
        first_prompt = lax.rem(me * ipd, prompts)
        if ipd % 8 == 0:
            first_prompt = pl.multiple_of(first_prompt, 8)
        cos_mine = tabs[0, pl.ds(first_prompt, ipd), :]
        sin_mine = tabs[1, pl.ds(first_prompt, ipd), :]
        for c in range(cols):
            value = total[c]
            if c <= group:
                value = value * cos_mine + pltpu.roll(value, HD // 2, 1) * sin_mine
            tr[:, c, :] = value
        for c in range(cols, 16):
            tr[:, c, :] = jnp.zeros((ipd, HD), F32)
        qg[me] = tr[...].astype(BF16)
        peers(lambda d: pool_copy(qg.at[me], qg.at[me], s2, r2, d).start())
        pl.loop(prompts // 2, prompts)(rotate_prompt)
        peers(lambda s: wait_from(qg.at[me], qg.at[s], s2, r2, s))

        slot_index = lax.broadcasted_iota(jnp.int32, (1, seq), 1) + me * seq

        batch = min(4, ipd)

        @pl.loop(1, n + 1)
        def _(k):
            d = lax.rem(me + k, n)
            v_copy(k).wait()
            slot = lax.rem(k, vslots)
            h = d // per_head
            first = lax.rem(d, per_head) * ipd
            tile = jnp.zeros((group, HD), F32)
            for i0 in range(0, ipd, batch):
                raw = []
                for i in range(i0, i0 + batch):
                    queries = qg[d, i][0:group]
                    scores = lax.dot_general(
                        queries, kbuf[first + i, h], (((1,), (1,)), ((), ())), preferred_element_type=F32
                    ) * scale
                    raw.append(jnp.where(slot_index < lens[first + i], scores, -1e30))
                stacked = jnp.concatenate(raw, 0)
                peak = jnp.maximum(jnp.max(stacked, -1, keepdims=True), -1e29)
                weights = jnp.exp(stacked - peak)
                sums = jnp.sum(weights, -1, keepdims=True)
                low = weights.astype(BF16)
                blended = []
                for j in range(batch):
                    i = i0 + j
                    rows = slice(j * group, (j + 1) * group)
                    blended.append(
                        jnp.dot(low[rows], vbuf[slot, i], preferred_element_type=F32)
                    )
                    tile = jnp.where(
                        lane_row == i, peak[rows], jnp.where(lane_row == i + HD // 2, sums[rows], tile)
                    )
                acc[d, i0 * group : (i0 + batch) * group] = jnp.concatenate(blended, 0).astype(BF16)
            ml[d] = tile

            @pl.when(k < n)
            def _():
                pool_copy(acc.at[d], acc_in.at[me], s3, r3, d).start()
                pool_copy(ml.at[d], ml_in.at[me], s4, r4, d).start()

            @pl.when(k + vslots < n + 1)
            def _():
                v_copy(k + vslots).start()

        own_tile = jnp.full((group, HD), -1e30, F32)
        own_values = []
        for i in range(ipd):
            row = qg[me, i].astype(F32)
            own = jnp.sum(row[0:group] * row[group : group + 1], -1, keepdims=True) * scale
            own_tile = jnp.where(lane_row == i, own, own_tile)
            own_values.append(row[group + 1 : group + 2])

        def wait_partial(s):
            wait_from(acc.at[s], acc_in.at[s], s3, r3, s)
            wait_from(ml.at[s], ml_in.at[s], s4, r4, s)

        peers(wait_partial)
        acc_in[me] = acc[me]
        ml_in[me] = ml[me]

        low_lane = lane_row < HD // 2
        top = lax.fori_loop(0, n, lambda s, t: jnp.maximum(t, ml_in[s]), own_tile, unroll=n <= 8)
        own_weight = jnp.where(low_lane, jnp.exp(own_tile - top), 0.0)

        def merge(s, carry):
            den, nums = carry
            tile = ml_in[s]
            factor = jnp.where(low_lane, jnp.exp(tile - top), 0.0)
            part_rows = acc_in[s].astype(F32)
            nums = [
                num + part_rows[i * group : (i + 1) * group] * factor[:, i : i + 1]
                for i, num in enumerate(nums)
            ]
            return den + pltpu.roll(tile, HD // 2, 1) * factor, nums

        nums = [own_weight[:, i : i + 1] * own_values[i] for i in range(ipd)]
        den, nums = lax.fori_loop(0, n, merge, (own_weight, nums), unroll=n <= 8)
        for i in range(ipd):
            atf[i] = nums[i] / den[:, i : i + 1]
        for j in range(group):
            ats[:, j * HD : (j + 1) * HD] = atf[:, j, :].astype(BF16)
        atg[me] = ats[...]
        peers(lambda d: pool_copy(ats, atg.at[me], s5, r5, d).start())
        peers(lambda s: wait_from(ats, atg.at[s], s5, r5, s))

        wo_copy.wait()
        part[...] = jnp.zeros_like(part)

        @pl.loop(0, lh)
        def _(h):
            rows = atg[pl.ds(h * per_head, per_head)].astype(F32).reshape(prompts, qw).astype(BF16)
            part[...] += jnp.dot(rows, wobuf[pl.ds(pl.multiple_of(h * qw, qw), qw), :], preferred_element_type=F32)

        def partner_copy(src, dst, idx):
            return pltpu.make_async_remote_copy(
                src_ref=src, dst_ref=dst, send_sem=hs.at[idx], recv_sem=hr.at[idx],
                device_id={"heads": other}, device_id_type=MESH,
            )

        part_copy = partner_copy(part, part_in, 0)
        part_copy.start()
        part_copy.wait_recv()
        mid = (my_cols + (part[...] + part_in[...])).astype(BF16).astype(F32)
        midf[0] = mid[0:half_rows]
        midf[1] = mid[half_rows:]
        mid_send[...] = midf[hd].astype(BF16)
        mg[hd, me] = mid_send[...]
        peers(lambda d: pool_copy(mid_send, mg.at[hd, me], s6, r6, d).start())
        peers(lambda s: wait_from(mid_send, mg.at[hd, s], s6, r6, s))
        half_copy = partner_copy(mg.at[hd], mg.at[hd], 1)
        half_copy.start()
        pltpu.make_async_remote_copy(
            src_ref=mg.at[other], dst_ref=mg.at[other], send_sem=hs.at[1], recv_sem=hr.at[1],
            device_id={"heads": other}, device_id_type=MESH,
        ).wait_recv()

        def squares(s, total):
            x = mg[:, s].astype(F32).reshape(prompts, cb)
            return total + jnp.sum(x * x, -1, keepdims=True)

        sq = lax.fori_loop(0, n, squares, jnp.zeros((prompts, 1), F32))
        inv_mid = lax.rsqrt(sq * (1.0 / d_model) + EPS)
        wg_copy.wait()
        wu_copy.wait()

        def ff(s, carry):
            g, u = carry
            x = (mg[:, s].astype(F32).reshape(prompts, cb) * inv_mid).astype(BF16)
            rows = pl.ds(pl.multiple_of(s * cb, cb), cb)
            nt = (((1,), (1,)), ((), ()))
            g = g + lax.dot_general(x, wgbuf[:, rows], nt, preferred_element_type=F32)
            u = u + lax.dot_general(x, wubuf[:, rows], nt, preferred_element_type=F32)
            return g, u

        zero = jnp.zeros((prompts, ffl), F32)
        gate, up = lax.fori_loop(0, n, ff, (zero, zero))
        ns[...] = (gate / (1.0 + jnp.exp(-gate)) * up).astype(BF16)

        per_block = wb // cb

        def dother_copy(d):
            return pltpu.make_async_remote_copy(
                src_ref=dpart.at[other, d], dst_ref=dother.at[d], send_sem=s7.at[d], recv_sem=r7.at[d],
                device_id={"heads": other}, device_id_type=MESH,
            )

        @pl.loop(0, nblocks)
        def _(b):
            down_copy(b).wait()
            slot = lax.rem(b, nslots)
            w = qkvbuf[slot, 0:ffl, :] if share else maybe_down[0][slot]
            res = jnp.dot(ns[...], w, preferred_element_type=F32)
            for t in range(per_block):
                d = b * per_block + t
                dpart[0, d] = res[0:half_rows, t * cb : (t + 1) * cb]
                dpart[1, d] = res[half_rows:, t * cb : (t + 1) * cb]
                dother_copy(d).start()

            @pl.when(b + nslots < nblocks)
            def _():
                down_copy(b + nslots).start()

        def reduce_and_send(d):
            dother_copy(d).wait_recv()
            ssum[d] = (dpart[hd, d] + dother[d]).astype(BF16)
            pool_copy(ssum.at[d], rsum.at[me], s8, r8, d).start()

        peers(reduce_and_send)
        dother_copy(me).wait_recv()
        final = dpart[hd, me] + dother[me]

        def add_final(k, total):
            s = lax.rem(me + k, n)
            wait_from(ssum.at[s], rsum.at[s], s8, r8, s)
            return total + rsum[s].astype(F32)

        final = lax.fori_loop(1, n, add_final, final)
        yb[hd] = (midf[hd] + final).astype(BF16)
        y_copy = partner_copy(yb.at[hd], yb.at[hd], 2)
        y_copy.start()
        pltpu.make_async_remote_copy(
            src_ref=yb.at[other], dst_ref=yb.at[other], send_sem=hs.at[2], recv_sem=hr.at[2],
            device_id={"heads": other}, device_id_type=MESH,
        ).wait_recv()
        out_ref[...] = yb[...].astype(F32).reshape(prompts, cb).astype(BF16)

        def drain(d):
            pool_copy(chunk.at[d], chunk_in.at[me], s1, r1, d).wait_send()
            pool_copy(qg.at[me], qg.at[me], s2, r2, d).wait_send()
            pool_copy(acc.at[d], acc_in.at[me], s3, r3, d).wait_send()
            pool_copy(ml.at[d], ml_in.at[me], s4, r4, d).wait_send()
            pool_copy(ats, atg.at[me], s5, r5, d).wait_send()
            pool_copy(mid_send, mg.at[hd, me], s6, r6, d).wait_send()
            pool_copy(ssum.at[d], rsum.at[me], s8, r8, d).wait_send()

        peers(drain)

        @pl.loop(0, n)
        def _(d):
            dother_copy(d).wait_send()

        part_copy.wait_send()
        half_copy.wait_send()
        y_copy.wait_send()

    return kernel


def per_device(
    n, hidden_in, key_cache, value_cache, positions, query_pos, lengths,
    query_weight, key_weight, value_weight, out_weight, gate_weight, up_weight, down_weight,
):
    prompts, d_model = hidden_in.shape
    lh, seq = key_cache.shape[1:3]
    cb = d_model // n
    ffl = gate_weight.shape[1]
    group = query_weight.shape[1] // key_weight.shape[1]
    qw = group * HD
    wb = max(cb, qw)
    nblocks = d_model // wb
    nslots = min(lh, nblocks)
    share = ffl % 16 == 0 and ffl <= cb and wb == qw
    vslots = 3
    items = prompts * lh
    ipd = items // n

    column = np.arange(HD) % (HD // 2)
    exponent = column.astype(np.float32) * np.float32(-2.0 * math.log(THETA) / HD)
    inverse = np.exp(exponent.astype(np.float64)).astype(np.float32)[None]
    first_end = HD // 8
    second_end = first_end + 3 * HD // 16
    which = np.where(column < first_end, 0, np.where(column < second_end, 1, 2))
    hit = (which[None] == np.arange(3)[:, None]).astype(np.float32)
    sel = jnp.asarray(np.concatenate([64.0 * hit, hit, np.zeros((2, HD), np.float32)], 0), BF16)

    kernel = make_kernel(n, prompts, lh, seq, d_model, ffl, group, wb, nslots, vslots, share)
    half = prompts // 2
    vm = pltpu.VMEM
    dma = pltpu.SemaphoreType.DMA
    scratch = [
        vm((prompts, lh, seq, HD), BF16),
        vm((vslots, ipd, seq, HD), BF16),
        vm((lh, cb, qw), BF16),
        vm(out_weight.shape, BF16),
        vm((ffl, d_model), BF16),
        vm((ffl, d_model), BF16),
        vm((n, group + 2, ipd, HD), F32),
        vm((n, group + 2, ipd, HD), F32),
        vm((ipd, 16, HD), F32),
        vm((n, ipd, 16, HD), BF16),
        vm((n, ipd * group, HD), BF16),
        vm((n, ipd * group, HD), BF16),
        vm((n, group, HD), F32),
        vm((n, group, HD), F32),
        vm((ipd, group, HD), F32),
        vm((ipd, qw), BF16),
        vm((n, ipd, qw), BF16),
        vm((prompts, cb), F32),
        vm((prompts, cb), F32),
        vm((2, half, cb), F32),
        vm((half, cb), BF16),
        vm((2, n, half, cb), BF16),
        vm((prompts, ffl), BF16),
        vm((2, n, half, cb), F32),
        vm((n, half, cb), F32),
        vm((n, half, cb), BF16),
        vm((n, half, cb), BF16),
        vm((2, half, cb), BF16),
        vm((2, prompts, HD), F32),
        dma((lh + 2,)),
        dma((prompts,)),
        dma((vslots,)),
        dma((3,)),
        dma((nslots,)),
    ] + [dma((n,)) for _ in range(16)] + [dma((3,)), dma((3,))]
    if not share:
        scratch.append(vm((nslots, ffl, wb), BF16))
    in_vmem = pl.BlockSpec(memory_space=pltpu.VMEM)
    in_any = pl.BlockSpec(memory_space=pl.ANY)
    return pl.pallas_call(
        kernel,
        out_shape=jax.ShapeDtypeStruct((prompts, cb), BF16),
        in_specs=[in_vmem] * 5 + [pl.BlockSpec(memory_space=pltpu.SMEM)] + [in_any] * 9,
        out_specs=in_vmem,
        scratch_shapes=scratch,
        compiler_params=pltpu.CompilerParams(
            collective_id=0, has_side_effects=True, vmem_limit_bytes=67043328
        ),
    )(
        hidden_in, positions, query_pos, sel, jnp.asarray(inverse), lengths, key_cache, value_cache,
        query_weight, key_weight, value_weight, out_weight, gate_weight.T, up_weight.T, down_weight,
    )


def solution(mesh):
    in_specs = (
        P("groups", None),
        P("groups", "heads", "pool", None),
        P("groups", "heads", "pool", None),
        P(None, "groups", "pool"),
        P(None, "groups"),
        P("groups"),
        P("pool", "heads"),
        P("pool", "heads"),
        P("pool", "heads"),
        P("heads", "pool"),
        P(None, ("pool", "heads")),
        P(None, ("pool", "heads")),
        P(("pool", "heads"), None),
    )
    return jax.shard_map(
        functools.partial(per_device, mesh.shape["pool"]),
        mesh=mesh,
        in_specs=in_specs,
        out_specs=P("groups", "pool"),
        check_vma=False,
    )
```
